512 devices in a mesh: unit: 2 (over y_1), row: 16 (over y_0, x, core), col: 16 (over z, y_2).
Axes of the slice: x: 4, y: 8 (y_0: 2, y_1: 2, y_2: 2; y = y_0 * 4 + y_1 * 2 + y_2), z: 8, core: 2. Of those that a mesh axis runs over, the one named last changes fastest.
Arguments:
- tracer: float32 [4, 128, 256, 256], P('unit', None, 'row', 'col'), parts along dimension 0, may hold values from -6 to 6
- symbol_x: float32 [128], replicated, may hold values from 0.3 to 3
- symbol_y: float32 [256], replicated, may hold values from 0.3 to 3
- symbol_z: float32 [256], replicated, may hold values from 0.3 to 3
Outputs:
- smoothed: float32 [4, 128, 256, 256], P('unit', None, 'row', 'col'), parts along dimension 0
The draws below stay inside these ranges and needn't reach their ends.
There are 2 independent parts, one for each index of `unit`. The reference program is written for one: setup_inputs(seed, part) draws one part's arguments, and reference() takes and returns one part's arrays. A program takes and returns all parts, laid end to end along the dimension named above; an argument that names none is the same for every part. Nothing has to cross between parts.
All inputs are finite; a program needn't handle non-finite values.
Results may differ from the reference program's by a relative error of at most 0.0003.
Values sent between devices are 32-bit elements.
No kernel may reach another device: no remote copies, remote signals or barrier semaphores. Data moves between devices by JAX's collectives and lax.ppermute only.
A program may use at most 64 MiB of HBM per device.

```python
import jax
import jax.numpy as jnp
from jax import lax

GRID_X = 128
GRID_Y = 256
GRID_Z = 256
FIELDS = 2


def levels(stream_key, extent, shards, smallest, top_value):
    def one(dim, shards_of):
        steps = jax.random.uniform(jax.random.fold_in(jax.random.fold_in(stream_key, 6), dim), (shards_of,), jnp.float32, smallest / len(shards), top_value / len(shards))
        return jnp.repeat(jnp.exp(steps), extent[dim] // shards_of).reshape((-1,) + (1,) * (len(extent) - dim - 1))

    factor_of = one(*shards[0])
    for cut in shards[1:]:
        factor_of = factor_of * one(*cut)
    return factor_of


def noise(key, extent, deviation, bound, split=(), dtype=jnp.bfloat16):
    level = levels(key, extent, split, -0.22, 0.18) if split else 1.0
    drawn = jax.random.normal(key, extent, jnp.float32) * deviation * level
    return jnp.minimum(jnp.maximum(drawn, -bound), bound).astype(dtype)


def setup_inputs(seed: int = 0, part: int = 0) -> dict:
    arg_keys = jax.random.split(jax.random.key(seed), 5)
    part_keys = jax.random.split(jax.random.fold_in(arg_keys[4], part), 5)
    return {
        "tracer": noise(part_keys[0], (FIELDS, GRID_X, GRID_Y, GRID_Z), 1.0, 6.0, ((2, 16), (3, 16)), jnp.float32),
        "symbol_x": jnp.clip(jax.random.uniform(arg_keys[1], (GRID_X,), jnp.float32, 0.3, 3.0), 0.3, 3.0),
        "symbol_y": jnp.clip(jax.random.uniform(arg_keys[2], (GRID_Y,), jnp.float32, 0.3, 3.0), 0.3, 3.0),
        "symbol_z": jnp.clip(jax.random.uniform(arg_keys[3], (GRID_Z,), jnp.float32, 0.3, 3.0), 0.3, 3.0),
    }


def mode_table(count):
    rank = jnp.arange(count)
    angle = jnp.pi / (4 * count) * ((2 * rank[:, None] + 1) * (2 * rank[None, :] + 1) % (8 * count)).astype(jnp.float32)
    return jnp.cos(angle) * (2.0 / count) ** 0.5

def to_modes(values, dim):
    moved = jnp.tensordot(values, mode_table(values.shape[dim]), axes=([dim], [0]), precision=lax.Precision.HIGHEST)
    return jnp.moveaxis(moved, -1, dim)

def reference(tracer, symbol_x, symbol_y, symbol_z):
    modes = tracer
    modes = to_modes(modes, 1)
    modes = to_modes(modes, 2)
    modes = to_modes(modes, 3)
    symbol = symbol_x[:, None, None] + symbol_y[None, :, None] + symbol_z[None, None, :]
    modes = modes * lax.rsqrt(symbol)
    smoothed = modes
    smoothed = to_modes(smoothed, 3)
    smoothed = to_modes(smoothed, 2)
    smoothed = to_modes(smoothed, 1)
    return smoothed
```

```python
import functools

import jax
import jax.numpy as jnp
import numpy as np
from jax import lax
from jax.experimental import pallas as pl
from jax.experimental.pallas import tpu as pltpu
from jax.sharding import PartitionSpec as P

LANES = 128
BLOCKS = 16
ROWS = 32


def mode_table(count):
    rank = np.arange(count)
    odd = (2 * rank[:, None] + 1) * (2 * rank[None, :] + 1) % (8 * count)
    return np.sqrt(2.0 / count) * np.cos(np.pi / (4 * count) * odd)


def halves(table):
    table = table.astype(np.float32)
    high = table.astype(jnp.bfloat16)
    low = (table - high.astype(np.float32)).astype(jnp.bfloat16)
    return np.stack([high, low])


def split(values):
    high = values.astype(jnp.bfloat16)
    return high, (values - high.astype(jnp.float32)).astype(jnp.bfloat16)


def dot(a, b):
    return jnp.dot(a, b, preferred_element_type=jnp.float32)


def times_table(values, table):
    high, low = split(values)
    return dot(high, table[0]) + (dot(low, table[0]) + dot(high, table[1]))


def table_times(table, values):
    high, low = split(values)
    return dot(table[0], high) + (dot(table[0], low) + dot(table[1], high))


def swap_bits(blocks, pairs):
    lane = lax.broadcasted_iota(jnp.int32, blocks[0].shape, 1)
    for block_bit, lane_bit in pairs:
        mask = (lane & lane_bit) == 0
        blocks = list(blocks)
        for i in range(len(blocks)):
            if i & block_bit:
                continue
            a, b = blocks[i], blocks[i | block_bit]
            blocks[i] = jnp.where(mask, a, pltpu.roll(b, lane_bit, 1))
            blocks[i | block_bit] = jnp.where(mask, pltpu.roll(a, LANES - lane_bit, 1), b)
    return blocks


X_SWAPS = ((1, 1), (2, 2), (4, 4), (8, 8))
Z_SWAPS = ((1, 16), (2, 32), (4, 64))


def x_first(a_ref, table_ref, o_ref):
    table = table_ref[...]
    blocks = [a_ref[pl.ds(k, ROWS, stride=BLOCKS), :] for k in range(BLOCKS)]
    values = times_table(jnp.concatenate(blocks, axis=0), table)
    blocks = [values[k * ROWS : (k + 1) * ROWS] for k in range(BLOCKS)]
    for k, block in enumerate(swap_bits(blocks, X_SWAPS)):
        o_ref[k] = block


def x_last(a_ref, table_ref, o_ref):
    table = table_ref[...]
    blocks = swap_bits([a_ref[k] for k in range(BLOCKS)], X_SWAPS)
    values = times_table(jnp.concatenate(blocks, axis=0), table)
    for k in range(BLOCKS):
        o_ref[pl.ds(k, ROWS, stride=BLOCKS), :] = values[k * ROWS : (k + 1) * ROWS]


def y_middle(a_ref, table_ref, o_ref):
    table = table_ref[...]
    half = ROWS // 2
    planes = [
        jnp.concatenate([a_ref[k, f * half : (f + 1) * half, :] for k in range(BLOCKS)], axis=0)
        for f in range(2)
    ]
    values = table_times(table, jnp.concatenate(planes, axis=1))
    for k in range(BLOCKS):
        for f in range(2):
            o_ref[k, f * half : (f + 1) * half, :] = values[
                k * half : (k + 1) * half, f * LANES : (f + 1) * LANES
            ]


def z_scaled(a_ref, table_ref, sx_ref, sy_ref, sz_ref, o_ref):
    table = table_ref[...]
    half = ROWS // 2
    row = lax.broadcasted_iota(jnp.int32, (half, LANES), 0)
    at_x, at_y = lax.axis_index("row") * 8, lax.axis_index("col") * half
    sy = jnp.full((half, LANES), sy_ref[at_y], jnp.float32)
    for k in range(1, half):
        sy = jnp.where(row == k, sy_ref[at_y + k], sy)
    sy = jnp.concatenate([sy, sy], axis=0)
    sxy = jnp.concatenate([sy + sx_ref[at_x + k] for k in range(8)], axis=0)
    symbol = jnp.concatenate([sxy, sxy], axis=1) + sz_ref[...]
    blocks = swap_bits([a_ref[k] for k in range(BLOCKS)], Z_SWAPS)
    values = jnp.concatenate(
        [jnp.concatenate(blocks[:8], axis=0), jnp.concatenate(blocks[8:], axis=0)], axis=1
    )
    values = times_table(values, table) * lax.rsqrt(symbol)
    values = times_table(values, table)
    blocks = [
        values[k * ROWS : (k + 1) * ROWS, h * LANES : (h + 1) * LANES]
        for h in range(2)
        for k in range(8)
    ]
    for k, block in enumerate(swap_bits(blocks, Z_SWAPS)):
        o_ref[k] = block


VMEM = pl.BlockSpec(memory_space=pltpu.VMEM)
SMEM = pl.BlockSpec(memory_space=pltpu.SMEM)
SPLIT = jax.ShapeDtypeStruct((BLOCKS, ROWS, LANES), jnp.float32)
FLAT = jax.ShapeDtypeStruct((BLOCKS * ROWS, LANES), jnp.float32)


def kernel(body, out, *specs):
    return pl.pallas_call(body, out_shape=out, in_specs=specs, out_specs=VMEM, name=body.__name__)


def shards(tracer, symbol_x, symbol_y, symbol_z):
    lane_x = (np.arange(LANES) % 16) * 8 + np.arange(LANES) // 16
    table_x = mode_table(LANES)
    first_x = jnp.asarray(halves(table_x[:, lane_x]))
    last_x = jnp.asarray(halves(table_x[lane_x, :]))
    table = jnp.asarray(halves(mode_table(256)))
    exchange = functools.partial(lax.all_to_all, split_axis=0, concat_axis=0, tiled=True)

    values = tracer.transpose(0, 2, 3, 1).reshape(FLAT.shape)
    values = kernel(x_first, SPLIT, VMEM, VMEM)(values, first_x)
    values = exchange(values, "row")
    values = kernel(y_middle, SPLIT, VMEM, VMEM)(values, table)
    values = exchange(values, "col")
    values = kernel(z_scaled, SPLIT, VMEM, VMEM, SMEM, SMEM, VMEM)(
        values, table, symbol_x, symbol_y, symbol_z.reshape(1, 256)
    )
    values = exchange(values, "col")
    values = kernel(y_middle, SPLIT, VMEM, VMEM)(values, table)
    values = exchange(values, "row")
    values = kernel(x_last, FLAT, VMEM, VMEM)(values, last_x)
    return values.reshape(2, 16, 16, LANES).transpose(0, 3, 1, 2)


def solution(mesh):
    in_specs = (P("unit", None, "row", "col"), P(), P(), P())
    out_specs = P("unit", None, "row", "col")
    return jax.shard_map(shards, mesh=mesh, in_specs=in_specs, out_specs=out_specs, check_vma=False)
```

```python
import functools

import jax
import jax.numpy as jnp
import numpy as np
from jax import lax
from jax.experimental import pallas as pl
from jax.experimental.pallas import tpu as pltpu
from jax.sharding import PartitionSpec as P

LANES = 128
ROWS = 512
LINES = 256


def mode_table(count):
    rank = np.arange(count)
    odd = (2 * rank[:, None] + 1) * (2 * rank[None, :] + 1) % (8 * count)
    return np.sqrt(2.0 / count) * np.cos(np.pi / (4 * count) * odd)


def halves(table):
    table = table.astype(np.float32)
    high = table.astype(jnp.bfloat16)
    low = (table - high.astype(np.float32)).astype(jnp.bfloat16)
    return np.stack([high, low])


def split(values):
    high = values.astype(jnp.bfloat16)
    return high, (values - high.astype(jnp.float32)).astype(jnp.bfloat16)


def dot(a, b):
    return jnp.dot(a, b, preferred_element_type=jnp.float32)


def times_table(values, table):
    high, low = split(values)
    return dot(high, table[0]) + (dot(low, table[0]) + dot(high, table[1]))


def table_times(table, values):
    high, low = split(values)
    return dot(table[0], high) + (dot(table[0], low) + dot(table[1], high))


def swap_bits(blocks, pairs):
    lane = lax.broadcasted_iota(jnp.int32, blocks[0].shape, 1)
    blocks = list(blocks)
    for block_bit, lane_bit in pairs:
        mask = (lane & lane_bit) == 0
        for i in range(len(blocks)):
            if i & block_bit:
                continue
            a, b = blocks[i], blocks[i | block_bit]
            blocks[i] = jnp.where(mask, a, pltpu.roll(b, lane_bit, 1))
            blocks[i | block_bit] = jnp.where(mask, pltpu.roll(a, LANES - lane_bit, 1), b)
    return blocks


SWAPS = ((2, 16), (4, 32), (8, 64))


def x_first(a_ref, table_ref, o_ref):
    columns = [a_ref[k * LANES : (k + 1) * LANES, :].T for k in range(4)]
    values = table_times(table_ref[...], jnp.concatenate(columns, axis=1))
    for k in range(4):
        o_ref[pl.ds((k // 2) * LINES + k % 2, LANES, stride=2), :] = values[
            :, k * LANES : (k + 1) * LANES
        ]


def x_last(a_ref, table_ref, o_ref):
    columns = [
        a_ref[pl.ds((k // 2) * LINES + k % 2, LANES, stride=2), :].T for k in range(4)
    ]
    o_ref[...] = times_table(jnp.concatenate(columns, axis=0), table_ref[...])


def plane(a_ref, in_ref, z_ref, out_ref, sx_ref, sy_ref, sz_ref, o_ref):
    at_x = (lax.axis_index("row") * 16 + lax.axis_index("col")) % LANES
    sy = [
        jnp.broadcast_to(sy_ref[:, k * LANES : (k + 1) * LANES], (LANES, LANES)).T
        for k in range(2)
    ]
    sy = jnp.concatenate(sy, axis=0) + sx_ref[at_x]
    scale = lax.rsqrt(jnp.concatenate([sy, sy], axis=1) + sz_ref[...])

    blocks = swap_bits([a_ref[pl.ds(k, 16, stride=32), :] for k in range(32)], SWAPS)
    order = [h + 2 * (yl + 8 * c) for c in range(2) for h in range(2) for yl in range(8)]
    values = jnp.concatenate(
        [jnp.concatenate([blocks[k] for k in order[c * 16 : c * 16 + 16]], axis=0) for c in range(2)],
        axis=1,
    )
    table = z_ref[...]
    values = table_times(in_ref[...], values)
    values = times_table(values, table) * scale
    values = times_table(values, table)
    values = table_times(out_ref[...], values)
    for n, k in enumerate(order):
        c, p = divmod(n, 16)
        blocks[k] = values[p * 16 : (p + 1) * 16, c * LANES : (c + 1) * LANES]
    for k, block in enumerate(swap_bits(blocks, SWAPS)):
        o_ref[pl.ds(k, 16, stride=32), :] = block


VMEM = pl.BlockSpec(memory_space=pltpu.VMEM)
SMEM = pl.BlockSpec(memory_space=pltpu.SMEM)
FLAT = jax.ShapeDtypeStruct((ROWS, LANES), jnp.float32)


def kernel(body, *specs):
    return pl.pallas_call(body, out_shape=FLAT, in_specs=specs, out_specs=VMEM, name=body.__name__)


def shards(tracer, symbol_x, symbol_y, symbol_z):
    line = (np.arange(LINES) % 16) * 16 + np.arange(LINES) // 16
    table_x = jnp.asarray(halves(mode_table(LANES)))
    table = mode_table(LINES)
    table_in, table_out = jnp.asarray(halves(table[:, line])), jnp.asarray(halves(table[line, :]))
    table = jnp.asarray(halves(table))
    exchange = functools.partial(
        lax.all_to_all, axis_name=("row", "col"), split_axis=0, concat_axis=0, tiled=True
    )

    values = tracer.transpose(0, 2, 3, 1).reshape(FLAT.shape)
    values = kernel(x_first, VMEM, VMEM)(values, table_x)
    values = exchange(values)
    values = kernel(plane, VMEM, VMEM, VMEM, VMEM, SMEM, VMEM, VMEM)(
        values, table_in, table, table_out, symbol_x, symbol_y.reshape(1, 256), symbol_z.reshape(1, 256)
    )
    values = exchange(values)
    values = kernel(x_last, VMEM, VMEM)(values, table_x)
    return values.reshape(2, 16, 16, LANES).transpose(0, 3, 1, 2)


def solution(mesh):
    in_specs = (P("unit", None, "row", "col"), P(), P(), P())
    out_specs = P("unit", None, "row", "col")
    return jax.shard_map(shards, mesh=mesh, in_specs=in_specs, out_specs=out_specs, check_vma=False)
```

```python
import functools

import jax
import jax.numpy as jnp
import numpy as np
from jax import lax
from jax.experimental import pallas as pl
from jax.experimental.pallas import tpu as pltpu
from jax.sharding import PartitionSpec as P

LANES = 128
ROWS = 512
LINES = 256
NEAR = ("x", "core")
FAR = ("y0", "z", "y2")
NEARS = 8
FARS = 32


def mode_table(count):
    rank = np.arange(count)
    odd = (2 * rank[:, None] + 1) * (2 * rank[None, :] + 1) % (8 * count)
    return np.sqrt(2.0 / count) * np.cos(np.pi / (4 * count) * odd)


def halves(table):
    table = table.astype(np.float32)
    high = table.astype(jnp.bfloat16)
    low = (table - high.astype(np.float32)).astype(jnp.bfloat16)
    return np.stack([high, low])


def split(values):
    high = values.astype(jnp.bfloat16)
    return high, (values - high.astype(jnp.float32)).astype(jnp.bfloat16)


def dot(a, b):
    return jnp.dot(a, b, preferred_element_type=jnp.float32)


def times_table(values, table):
    high, low = split(values)
    return dot(high, table[0]) + (dot(low, table[0]) + dot(high, table[1]))


def table_times(table, values):
    high, low = split(values)
    return dot(table[0], high) + (dot(table[0], low) + dot(table[1], high))


def swap_bits(blocks, pairs):
    lane = lax.broadcasted_iota(jnp.int32, blocks[0].shape, 1)
    blocks = list(blocks)
    for block_bit, lane_bit in pairs:
        mask = (lane & lane_bit) == 0
        for i in range(len(blocks)):
            if i & block_bit:
                continue
            a, b = blocks[i], blocks[i | block_bit]
            blocks[i] = jnp.where(mask, a, pltpu.roll(b, lane_bit, 1))
            blocks[i | block_bit] = jnp.where(mask, pltpu.roll(a, LANES - lane_bit, 1), b)
    return blocks


SWAPS = ((2, 16), (4, 32), (8, 64))


def x_first(a_ref, table_ref, o_ref):
    columns = [a_ref[k * LANES : (k + 1) * LANES, :].T for k in range(4)]
    values = table_times(table_ref[...], jnp.concatenate(columns, axis=1))
    for k in range(4):
        o_ref[pl.ds((k // 2) * LINES + k % 2, LANES, stride=2), :] = values[
            :, k * LANES : (k + 1) * LANES
        ]


def x_last(a_ref, table_ref, o_ref):
    columns = [
        a_ref[pl.ds((k // 2) * LINES + k % 2, LANES, stride=2), :].T for k in range(4)
    ]
    o_ref[...] = times_table(jnp.concatenate(columns, axis=0), table_ref[...])


def to_far(a_ref, o_ref):
    for near in range(NEARS):
        for h in range(2):
            o_ref[pl.ds(near * 2 + h, FARS, stride=2 * NEARS), :] = a_ref[
                pl.ds(near * 2 * FARS + h, FARS, stride=2), :
            ]


def to_near(a_ref, o_ref):
    for near in range(NEARS):
        for h in range(2):
            o_ref[pl.ds(near * 2 * FARS + h, FARS, stride=2), :] = a_ref[
                pl.ds(near * 2 + h, FARS, stride=2 * NEARS), :
            ]


def plane(a_ref, in_ref, z_ref, out_ref, sx_ref, sy_ref, sz_ref, o_ref):
    at_x = (lax.axis_index(NEAR) * FARS + lax.axis_index(FAR)) % LANES
    sy = [
        jnp.broadcast_to(sy_ref[:, k * LANES : (k + 1) * LANES], (LANES, LANES)).T
        for k in range(2)
    ]
    sy = jnp.concatenate(sy, axis=0) + sx_ref[at_x]
    scale = lax.rsqrt(jnp.concatenate([sy, sy], axis=1) + sz_ref[...])

    starts = [(k // 2) * 16 + k % 2 for k in range(32)]
    blocks = [
        jnp.concatenate([a_ref[pl.ds(s + y0 * LINES, 8, stride=2), :] for y0 in range(2)], axis=0)
        for s in starts
    ]
    blocks = swap_bits(blocks, SWAPS)
    order = [h + 2 * (yl + 8 * c) for c in range(2) for h in range(2) for yl in range(8)]
    values = jnp.concatenate(
        [jnp.concatenate([blocks[k] for k in order[c * 16 : c * 16 + 16]], axis=0) for c in range(2)],
        axis=1,
    )
    table = z_ref[...]
    values = table_times(in_ref[...], values)
    values = times_table(values, table) * scale
    values = times_table(values, table)
    values = table_times(out_ref[...], values)
    for n, k in enumerate(order):
        c, p = divmod(n, 16)
        blocks[k] = values[p * 16 : (p + 1) * 16, c * LANES : (c + 1) * LANES]
    for s, block in zip(starts, swap_bits(blocks, SWAPS)):
        for y0 in range(2):
            o_ref[pl.ds(s + y0 * LINES, 8, stride=2), :] = block[y0 * 8 : y0 * 8 + 8]


VMEM = pl.BlockSpec(memory_space=pltpu.VMEM)
SMEM = pl.BlockSpec(memory_space=pltpu.SMEM)
FLAT = jax.ShapeDtypeStruct((ROWS, LANES), jnp.float32)


def kernel(body, *specs):
    return pl.pallas_call(body, out_shape=FLAT, in_specs=specs, out_specs=VMEM, name=body.__name__)


def shards(tracer, symbol_x, symbol_y, symbol_z):
    line = (np.arange(LINES) % 16) * 16 + np.arange(LINES) // 16
    table_x = jnp.asarray(halves(mode_table(LANES)))
    table = mode_table(LINES)
    table_in, table_out = jnp.asarray(halves(table[:, line])), jnp.asarray(halves(table[line, :]))
    table = jnp.asarray(halves(table))
    exchange = functools.partial(lax.all_to_all, split_axis=0, concat_axis=0, tiled=True)

    values = tracer.transpose(0, 2, 3, 1).reshape(FLAT.shape)
    values = kernel(x_first, VMEM, VMEM)(values, table_x)
    values = exchange(values, NEAR)
    values = kernel(to_far, VMEM)(values)
    values = exchange(values, FAR)
    values = kernel(plane, VMEM, VMEM, VMEM, VMEM, SMEM, VMEM, VMEM)(
        values, table_in, table, table_out, symbol_x, symbol_y.reshape(1, 256), symbol_z.reshape(1, 256)
    )
    values = exchange(values, FAR)
    values = kernel(to_near, VMEM)(values)
    values = exchange(values, NEAR)
    values = kernel(x_last, VMEM, VMEM)(values, table_x)
    return values.reshape(2, 16, 16, LANES).transpose(0, 3, 1, 2)


def solution(mesh):
    axes = ("unit", "y0", "x", "core", "z", "y2")
    mesh = jax.sharding.Mesh(mesh.devices.reshape(2, 2, 4, 2, 8, 2), axes)
    spec = P("unit", None, ("y0", "x", "core"), ("z", "y2"))
    return jax.shard_map(
        shards, mesh=mesh, in_specs=(spec, P(), P(), P()), out_specs=spec, check_vma=False
    )
```
